16 devices in a mesh: mp: 2 (over z), dp: 8 (over y, x, core).
Axes of the slice: x: 2, y: 2, z: 2, core: 2. Of those that a mesh axis runs over, the one named last changes fastest.
Arguments:
- a_mat: bfloat16 [4096, 65536], P(('mp', 'dp'))
- b_mat: bfloat16 [65536, 4096], P(('mp', 'dp'))
Outputs:
- output: bfloat16 [4096, 4096], P(('mp', 'dp'))
All inputs are finite; a program needn't handle non-finite values.
Results may differ from the reference program's by a relative error of at most 0.001.
Values are sent between devices in bfloat16 or wider.
A program may use at most 1 GiB of HBM per device.

```python
import jax
import jax.numpy as jnp

M_DIM = 4096
N_DIM = 4096
TOKENS = 65536


def setup_inputs(seed: int = 0) -> dict:
    root_key = jax.random.key(seed)
    key_a, key_b = jax.random.split(root_key)
    a_mat = jax.random.normal(key_a, (M_DIM, TOKENS), jnp.float32)
    b_mat = jax.random.normal(key_b, (TOKENS, N_DIM), jnp.float32) * (TOKENS ** -0.5)
    return {"a_mat": a_mat.astype(jnp.bfloat16), "b_mat": b_mat.astype(jnp.bfloat16)}


def reference(a_mat, b_mat):
    return jnp.dot(a_mat, b_mat, preferred_element_type=jnp.float32).astype(jnp.bfloat16)
```

```python
import jax
import jax.numpy as jnp
from jax import lax
from jax.experimental import pallas as pl
from jax.experimental.pallas import tpu as pltpu
from jax.sharding import PartitionSpec as P

MESH = pl.DeviceIdType.MESH
CHIPS = 8
STEPS = 4
COLS = 512
TWO_HOP = ((3, 1, 2), (6, 2, 4), (5, 4, 1))


def flip(chip, axis):
    return chip + axis * (1 - 2 * ((chip // axis) % 2))


def across(chip, rel):
    for axis in (1, 2, 4):
        if rel & axis:
            chip = flip(chip, axis)
    return chip


def axes_of(unit):
    turns = [(unit + k) % 3 for k in range(3)]
    return [1 + turn + turn // 2 for turn in turns]


def wait_bytes(ref, sem):
    pltpu.make_async_copy(ref, ref, sem).wait()


def kernel(
    a_ref, b_ref,
    c_ref, a_in, a_via, b_in, part, part_in,
    a_vm, b_vm, prod, total, fetched, sum_in, last_in, c_vm,
    a_out_sem, a_in_sem, via_sem, b_sem, a_load, b_load, prod_sem,
    part_out_sem, part_in_sem, sum_out_sem, sum_in_sem, last_out_sem, last_in_sem,
    fetch_sem, c_sem,
):
    mp, dp = lax.axis_index("mp"), lax.axis_index("dp")
    chip, core = mp * 4 + dp // 2, dp % 2
    rows = a_ref.shape[0]
    depth, width = b_ref.shape
    span = 2 * depth
    step_rows = rows // STEPS
    blocks = width // COLS
    units = STEPS * blocks

    def device(chip_no, core_no):
        return (chip_no // 4, (chip_no % 4) * 2 + core_no)

    def send(src, dst, send_sem, recv_sem, chip_no, core_no=core):
        pltpu.make_async_remote_copy(
            src, dst, send_sem, recv_sem, device_id=device(chip_no, core_no), device_id_type=MESH
        ).start()

    def chunk(step):
        return pl.ds(pl.multiple_of(step * step_rows, step_rows), step_rows)

    def a_block(step, rel):
        first = pl.multiple_of(across(chip, rel) * span, span)
        return a_ref.at[chunk(step), pl.ds(first, span)]

    def send_first(step):
        send(a_block(step, 7), a_in.at[6, chunk(step)], a_out_sem.at[6], a_in_sem.at[step], across(chip, 7))
        for k, (rel, first, _) in enumerate(TWO_HOP):
            send(a_block(step, rel), a_via.at[k, chunk(step)], a_out_sem.at[k], via_sem.at[step, k], flip(chip, first))
        for k, rel in enumerate((1, 2, 4)):
            send(a_block(step, rel), a_in.at[rel - 1, chunk(step)], a_out_sem.at[3 + k], a_in_sem.at[step], flip(chip, rel))

    def forward(step):
        for k, (rel, _, second) in enumerate(TWO_HOP):
            block = a_via.at[k, chunk(step)]
            wait_bytes(block, via_sem.at[step, k])
            send(block, a_in.at[rel - 1, chunk(step)], a_out_sem.at[7 + k], a_in_sem.at[step], flip(chip, second))

    barrier = pltpu.get_barrier_semaphore()
    for rel in (1, 2, 4, 7):
        pl.semaphore_signal(barrier, inc=1, device_id=device(across(chip, rel), core), device_id_type=MESH)
    pl.semaphore_signal(barrier, inc=1, device_id=device(chip, 1 - core), device_id_type=MESH)
    pl.semaphore_wait(barrier, 5)

    send_first(0)
    send(b_ref, b_in, b_sem.at[0], b_sem.at[1], chip, 1 - core)
    send_first(1)
    for step in range(2):
        forward(step)
        send_first(step + 2)

    def b_copies(block, slot):
        cols = pl.ds(pl.multiple_of(block * COLS, COLS), COLS)
        own = pl.ds(pl.multiple_of(core * depth, depth), depth)
        other = pl.ds(pl.multiple_of((1 - core) * depth, depth), depth)
        return (
            pltpu.make_async_copy(b_ref.at[:, cols], b_vm.at[slot, own], b_load.at[slot]),
            pltpu.make_async_copy(b_in.at[:, cols], b_vm.at[slot, other], b_load.at[slot]),
        )

    wait_bytes(b_in, b_sem.at[1])
    for copy in b_copies(0, 0):
        copy.start()

    def rel_rows(rel):
        return pl.ds(pl.multiple_of(rel * step_rows, step_rows), step_rows)

    def send_parts(unit):
        first, second, third = axes_of(unit)
        slot = unit % 2
        pltpu.make_async_copy(prod.at[slot], part.at[unit], prod_sem.at[slot]).wait()
        for k in range(4):
            rel = first + second * (k // 2) + third * (k % 2)
            send(part.at[unit, rel_rows(rel)], part_in.at[unit, k], part_out_sem, part_in_sem.at[unit], flip(chip, first))

    def multiply(step, _):
        @pl.when((step >= 1) & (step + 1 < STEPS))
        def _():
            forward(step + 1)

        wait_bytes(a_in.at[:, chunk(step)], a_in_sem.at[step])
        pltpu.make_async_copy(a_block(step, 0), a_vm.at[rel_rows(0)], a_load).start()
        for rel in range(1, CHIPS):
            pltpu.make_async_copy(a_in.at[rel - 1, chunk(step)], a_vm.at[rel_rows(rel)], a_load).start()
        wait_bytes(a_vm, a_load)

        def one_unit(block, _):
            unit = step * blocks + block
            slot = unit % 2

            @pl.when(unit + 1 < units)
            def _():
                for copy in b_copies((block + 1) % blocks, 1 - slot):
                    copy.start()

            wait_bytes(b_vm.at[slot], b_load.at[slot])
            prod[slot] = jnp.dot(a_vm[...], b_vm[slot], preferred_element_type=jnp.float32)
            pltpu.make_async_copy(prod.at[slot], part.at[unit], prod_sem.at[slot]).start()

            @pl.when(unit >= 1)
            def _():
                send_parts(unit - 1)

            return 0

        return lax.fori_loop(0, blocks, one_unit, 0)

    lax.fori_loop(0, STEPS, multiply, 0)
    send_parts(units - 1)

    def fetch(unit):
        _, second, third = axes_of(unit)
        slot = unit % 2
        wait_bytes(part_in.at[unit], part_in_sem.at[unit])
        pltpu.make_async_copy(part_in.at[unit], fetched.at[slot, 0], fetch_sem.at[slot]).start()
        for k in range(4):
            rel = second * (k // 2) + third * (k % 2)
            pltpu.make_async_copy(
                part.at[unit, rel_rows(rel)], fetched.at[slot, 1, k], fetch_sem.at[slot]
            ).start()

    fetch(0)

    def add_first(unit, _):
        _, second, _ = axes_of(unit)
        slot = unit % 2

        @pl.when(unit + 1 < units)
        def _():
            fetch(unit + 1)

        wait_bytes(fetched.at[slot], fetch_sem.at[slot])
        total[unit] = fetched[slot, 0] + fetched[slot, 1]
        for k in range(2):
            send(total.at[unit, 2 + k], sum_in.at[unit, k], sum_out_sem, sum_in_sem.at[unit], flip(chip, second))
        return 0

    lax.fori_loop(0, units, add_first, 0)

    def add_second(unit, _):
        _, _, third = axes_of(unit)
        wait_bytes(sum_in.at[unit], sum_in_sem.at[unit])
        for k in (1, 0):
            total[unit, k] = total[unit, k] + sum_in[unit, k]
        send(total.at[unit, 1], last_in.at[unit], last_out_sem, last_in_sem.at[unit], flip(chip, third))
        return 0

    lax.fori_loop(0, units, add_second, 0)

    def add_last(unit, _):
        wait_bytes(last_in.at[unit], last_in_sem.at[unit])
        c_vm[unit] = (total[unit, 0] + last_in[unit]).astype(c_vm.dtype)
        cols = pl.ds(pl.multiple_of((unit % blocks) * COLS, COLS), COLS)
        pltpu.make_async_copy(c_vm.at[unit], c_ref.at[chunk(unit // blocks), cols], c_sem).start()
        return 0

    lax.fori_loop(0, units, add_last, 0)

    wait_bytes(c_vm, c_sem)
    for k in range(10):
        wait_bytes(a_in.at[0], a_out_sem.at[k])
    wait_bytes(b_ref, b_sem.at[0])
    wait_bytes(part_in, part_out_sem)
    wait_bytes(sum_in, sum_out_sem)
    wait_bytes(last_in, last_out_sem)


def local_product(a_rows, b_rows):
    rows, inner = a_rows.shape
    depth, width = b_rows.shape
    span = inner // CHIPS
    step_rows = rows // STEPS
    units = STEPS * (width // COLS)
    f32, bf16 = jnp.float32, a_rows.dtype
    tile = (step_rows, COLS)
    dma = pltpu.SemaphoreType.DMA
    outs = pl.pallas_call(
        kernel,
        out_shape=[
            jax.ShapeDtypeStruct((rows, width), bf16),
            jax.ShapeDtypeStruct((CHIPS - 1, rows, span), bf16),
            jax.ShapeDtypeStruct((len(TWO_HOP), rows, span), bf16),
            jax.ShapeDtypeStruct((depth, width), bf16),
            jax.ShapeDtypeStruct((units, CHIPS * step_rows, COLS), f32),
            jax.ShapeDtypeStruct((units, 4) + tile, f32),
        ],
        in_specs=[pl.BlockSpec(memory_space=pl.ANY)] * 2,
        out_specs=[pl.BlockSpec(memory_space=pl.ANY)] * 6,
        scratch_shapes=[
            pltpu.VMEM((CHIPS * step_rows, span), bf16),
            pltpu.VMEM((2, span, COLS), bf16),
            pltpu.VMEM((2, CHIPS * step_rows, COLS), f32),
            pltpu.VMEM((units, 4) + tile, f32),
            pltpu.VMEM((2, 2, 4) + tile, f32),
            pltpu.VMEM((units, 2) + tile, f32),
            pltpu.VMEM((units,) + tile, f32),
            pltpu.VMEM((units,) + tile, bf16),
            dma((10,)), dma((STEPS,)), dma((STEPS, len(TWO_HOP))), dma((2,)), dma, dma((2,)), dma((2,)),
            dma, dma((units,)), dma, dma((units,)), dma, dma((units,)),
            dma((2,)), dma,
        ],
        compiler_params=pltpu.CompilerParams(
            collective_id=0, has_side_effects=True, vmem_limit_bytes=67043328
        ),
    )(a_rows, b_rows)
    return outs[0]


def solution(mesh):
    return jax.shard_map(
        local_product,
        mesh=mesh,
        in_specs=(P(("mp", "dp"), None), P(("mp", "dp"), None)),
        out_specs=P(("mp", "dp"), None),
        check_vma=False,
    )
```

```python
import jax
import jax.numpy as jnp
from jax import lax
from jax.experimental import pallas as pl
from jax.experimental.pallas import tpu as pltpu
from jax.sharding import PartitionSpec as P

MESH = pl.DeviceIdType.MESH
CHIPS = 8
STEPS = 4
COLS = 512
TWO_HOP = ((3, 1, 2), (6, 2, 4), (5, 4, 1))


def flip(chip, axis):
    return chip + axis * (1 - 2 * ((chip // axis) % 2))


def across(chip, rel):
    for axis in (1, 2, 4):
        if rel & axis:
            chip = flip(chip, axis)
    return chip


def axes_of(unit):
    turns = [(unit + k) % 3 for k in range(3)]
    first, second, third = [1 + turn + turn // 2 for turn in turns]
    swap = 1 // (unit + 1)
    return first, second + swap * (third - second), third + swap * (second - third)


def wait_bytes(ref, sem):
    pltpu.make_async_copy(ref, ref, sem).wait()


def kernel(
    a_ref, b_ref,
    c_ref, a_in, a_via, b_in, part, part_in,
    a_vm, b_vm, prod, total, fetched, sum_in, last_in, c_vm,
    a_out_sem, a_in_sem, via_sem, b_sem, a_load, b_load, prod_sem,
    part_out_sem, part_in_sem, sum_out_sem, sum_in_sem, last_out_sem, last_in_sem,
    fetch_sem, c_sem,
):
    mp, dp = lax.axis_index("mp"), lax.axis_index("dp")
    chip, core = mp * 4 + dp // 2, dp % 2
    rows = a_ref.shape[0]
    depth, width = b_ref.shape
    span = 2 * depth
    step_rows = rows // STEPS
    blocks = width // COLS
    units = STEPS * blocks

    def device(chip_no, core_no):
        return (chip_no // 4, (chip_no % 4) * 2 + core_no)

    def send(src, dst, send_sem, recv_sem, chip_no, core_no=core):
        pltpu.make_async_remote_copy(
            src, dst, send_sem, recv_sem, device_id=device(chip_no, core_no), device_id_type=MESH
        ).start()

    def chunk(step):
        return pl.ds(pl.multiple_of(step * step_rows, step_rows), step_rows)

    def a_block(step, rel):
        first = pl.multiple_of(across(chip, rel) * span, span)
        return a_ref.at[chunk(step), pl.ds(first, span)]

    def send_first(step):
        send(a_block(step, 7), a_in.at[6, chunk(step)], a_out_sem.at[6], a_in_sem.at[step], across(chip, 7))
        for k, (rel, first, _) in enumerate(TWO_HOP):
            send(a_block(step, rel), a_via.at[k, chunk(step)], a_out_sem.at[k], via_sem.at[step, k], flip(chip, first))
        for k, rel in enumerate((1, 2, 4)):
            send(a_block(step, rel), a_in.at[rel - 1, chunk(step)], a_out_sem.at[3 + k], a_in_sem.at[step], flip(chip, rel))

    def forward(step):
        for k, (rel, _, second) in enumerate(TWO_HOP):
            block = a_via.at[k, chunk(step)]
            wait_bytes(block, via_sem.at[step, k])
            send(block, a_in.at[rel - 1, chunk(step)], a_out_sem.at[7 + k], a_in_sem.at[step], flip(chip, second))

    barrier = pltpu.get_barrier_semaphore()
    for rel in (1, 2, 4, 7):
        pl.semaphore_signal(barrier, inc=1, device_id=device(across(chip, rel), core), device_id_type=MESH)
    pl.semaphore_signal(barrier, inc=1, device_id=device(chip, 1 - core), device_id_type=MESH)
    pl.semaphore_wait(barrier, 5)

    send_first(0)
    send(b_ref, b_in, b_sem.at[0], b_sem.at[1], chip, 1 - core)
    send_first(1)
    for step in range(2):
        forward(step)
        send_first(step + 2)

    def b_copies(block, slot):
        cols = pl.ds(pl.multiple_of(block * COLS, COLS), COLS)
        own = pl.ds(pl.multiple_of(core * depth, depth), depth)
        other = pl.ds(pl.multiple_of((1 - core) * depth, depth), depth)
        return (
            pltpu.make_async_copy(b_ref.at[:, cols], b_vm.at[slot, own], b_load.at[slot]),
            pltpu.make_async_copy(b_in.at[:, cols], b_vm.at[slot, other], b_load.at[slot]),
        )

    wait_bytes(b_in, b_sem.at[1])
    for copy in b_copies(0, 0):
        copy.start()

    def rel_rows(rel):
        return pl.ds(pl.multiple_of(rel * step_rows, step_rows), step_rows)

    def send_parts(unit):
        first, second, third = axes_of(unit)
        slot = unit % 2
        pltpu.make_async_copy(prod.at[slot], part.at[unit], prod_sem.at[slot]).wait()
        for k in range(4):
            rel = first + second * (k // 2) + third * (k % 2)
            send(part.at[unit, rel_rows(rel)], part_in.at[unit, k], part_out_sem, part_in_sem.at[unit], flip(chip, first))

    def multiply(step, _):
        @pl.when((step >= 1) & (step + 1 < STEPS))
        def _():
            forward(step + 1)

        wait_bytes(a_in.at[:, chunk(step)], a_in_sem.at[step])
        pltpu.make_async_copy(a_block(step, 0), a_vm.at[rel_rows(0)], a_load).start()
        for rel in range(1, CHIPS):
            pltpu.make_async_copy(a_in.at[rel - 1, chunk(step)], a_vm.at[rel_rows(rel)], a_load).start()
        wait_bytes(a_vm, a_load)

        def one_unit(block, _):
            unit = step * blocks + block
            slot = unit % 2

            @pl.when(unit + 1 < units)
            def _():
                for copy in b_copies((block + 1) % blocks, 1 - slot):
                    copy.start()

            wait_bytes(b_vm.at[slot], b_load.at[slot])
            prod[slot] = jnp.dot(a_vm[...], b_vm[slot], preferred_element_type=jnp.float32)
            pltpu.make_async_copy(prod.at[slot], part.at[unit], prod_sem.at[slot]).start()

            @pl.when(unit >= 1)
            def _():
                send_parts(unit - 1)

            return 0

        return lax.fori_loop(0, blocks, one_unit, 0)

    lax.fori_loop(0, STEPS, multiply, 0)
    send_parts(units - 1)

    def fetch(unit):
        _, second, third = axes_of(unit)
        slot = unit % 2
        wait_bytes(part_in.at[unit], part_in_sem.at[unit])
        pltpu.make_async_copy(part_in.at[unit], fetched.at[slot, 0], fetch_sem.at[slot]).start()
        for k in range(4):
            rel = second * (k // 2) + third * (k % 2)
            pltpu.make_async_copy(
                part.at[unit, rel_rows(rel)], fetched.at[slot, 1, k], fetch_sem.at[slot]
            ).start()

    fetch(0)

    def add_first(unit, _):
        _, second, _ = axes_of(unit)
        slot = unit % 2

        @pl.when(unit + 1 < units)
        def _():
            fetch(unit + 1)

        wait_bytes(fetched.at[slot], fetch_sem.at[slot])
        for k in (2, 3):
            total[unit, k] = fetched[slot, 0, k] + fetched[slot, 1, k]
            send(total.at[unit, k], sum_in.at[unit, k - 2], sum_out_sem, sum_in_sem.at[unit], flip(chip, second))
        for k in (0, 1):
            total[unit, k] = fetched[slot, 0, k] + fetched[slot, 1, k]
        return 0

    lax.fori_loop(0, units, add_first, 0)

    def add_second(unit, _):
        _, _, third = axes_of(unit)
        wait_bytes(sum_in.at[unit], sum_in_sem.at[unit])
        total[unit, 1] = total[unit, 1] + sum_in[unit, 1]
        send(total.at[unit, 1], last_in.at[unit], last_out_sem, last_in_sem.at[unit], flip(chip, third))
        total[unit, 0] = total[unit, 0] + sum_in[unit, 0]
        return 0

    lax.fori_loop(0, units, add_second, 0)

    def add_last(unit, _):
        wait_bytes(last_in.at[unit], last_in_sem.at[unit])
        c_vm[unit] = (total[unit, 0] + last_in[unit]).astype(c_vm.dtype)
        cols = pl.ds(pl.multiple_of((unit % blocks) * COLS, COLS), COLS)
        pltpu.make_async_copy(c_vm.at[unit], c_ref.at[chunk(unit // blocks), cols], c_sem).start()
        return 0

    lax.fori_loop(0, units, add_last, 0)

    wait_bytes(c_vm, c_sem)
    for k in range(10):
        wait_bytes(a_in.at[0], a_out_sem.at[k])
    wait_bytes(b_ref, b_sem.at[0])
    wait_bytes(part_in, part_out_sem)
    wait_bytes(sum_in, sum_out_sem)
    wait_bytes(last_in, last_out_sem)


def local_product(a_rows, b_rows):
    rows, inner = a_rows.shape
    depth, width = b_rows.shape
    span = inner // CHIPS
    step_rows = rows // STEPS
    units = STEPS * (width // COLS)
    f32, bf16 = jnp.float32, a_rows.dtype
    tile = (step_rows, COLS)
    dma = pltpu.SemaphoreType.DMA
    outs = pl.pallas_call(
        kernel,
        out_shape=[
            jax.ShapeDtypeStruct((rows, width), bf16),
            jax.ShapeDtypeStruct((CHIPS - 1, rows, span), bf16),
            jax.ShapeDtypeStruct((len(TWO_HOP), rows, span), bf16),
            jax.ShapeDtypeStruct((depth, width), bf16),
            jax.ShapeDtypeStruct((units, CHIPS * step_rows, COLS), f32),
            jax.ShapeDtypeStruct((units, 4) + tile, f32),
        ],
        in_specs=[pl.BlockSpec(memory_space=pl.ANY)] * 2,
        out_specs=[pl.BlockSpec(memory_space=pl.ANY)] * 6,
        scratch_shapes=[
            pltpu.VMEM((CHIPS * step_rows, span), bf16),
            pltpu.VMEM((2, span, COLS), bf16),
            pltpu.VMEM((2, CHIPS * step_rows, COLS), f32),
            pltpu.VMEM((units, 4) + tile, f32),
            pltpu.VMEM((2, 2, 4) + tile, f32),
            pltpu.VMEM((units, 2) + tile, f32),
            pltpu.VMEM((units,) + tile, f32),
            pltpu.VMEM((units,) + tile, bf16),
            dma((10,)), dma((STEPS,)), dma((STEPS, len(TWO_HOP))), dma((2,)), dma, dma((2,)), dma((2,)),
            dma, dma((units,)), dma, dma((units,)), dma, dma((units,)),
            dma((2,)), dma,
        ],
        compiler_params=pltpu.CompilerParams(
            collective_id=0, has_side_effects=True, vmem_limit_bytes=67043328
        ),
    )(a_rows, b_rows)
    return outs[0]


def solution(mesh):
    return jax.shard_map(
        local_product,
        mesh=mesh,
        in_specs=(P(("mp", "dp"), None), P(("mp", "dp"), None)),
        out_specs=P(("mp", "dp"), None),
        check_vma=False,
    )
```

```python
import jax
import jax.numpy as jnp
from jax import lax
from jax.experimental import pallas as pl
from jax.experimental.pallas import tpu as pltpu
from jax.sharding import PartitionSpec as P

MESH = pl.DeviceIdType.MESH
CHIPS = 8
STEPS = 4
COLS = 512
TWO_HOP = ((3, 1, 2), (6, 2, 4), (5, 4, 1))


def flip(chip, axis):
    return chip + axis * (1 - 2 * ((chip // axis) % 2))


def across(chip, rel):
    for axis in (1, 2, 4):
        if rel & axis:
            chip = flip(chip, axis)
    return chip


def axes_of(unit):
    turns = [(unit + k) % 3 for k in range(3)]
    first, second, third = [1 + turn + turn // 2 for turn in turns]
    swap = 1 // (unit + 1)
    return first, second + swap * (third - second), third + swap * (second - third)


def wait_bytes(ref, sem):
    pltpu.make_async_copy(ref, ref, sem).wait()


def kernel(
    a_ref, b_ref,
    c_ref, a_in, a_via, b_in, part, part_in,
    a_vm, b_vm, prod, total, fetched, sum_in, last_in, c_vm,
    a_out_sem, a_in_sem, via_sem, b_sem, a_load, b_load, prod_sem,
    part_out_sem, part_in_sem, sum_out_sem, sum_in_sem, last_out_sem, last_in_sem,
    fetch_sem, c_sem,
):
    mp, dp = lax.axis_index("mp"), lax.axis_index("dp")
    chip, core = mp * 4 + dp // 2, dp % 2
    rows = a_ref.shape[0]
    depth, width = b_ref.shape
    span = 2 * depth
    step_rows = rows // STEPS
    blocks = width // COLS
    units = STEPS * blocks

    def device(chip_no, core_no):
        return (chip_no // 4, (chip_no % 4) * 2 + core_no)

    def send(src, dst, send_sem, recv_sem, chip_no, core_no=core):
        pltpu.make_async_remote_copy(
            src, dst, send_sem, recv_sem, device_id=device(chip_no, core_no), device_id_type=MESH
        ).start()

    def chunk(step):
        return pl.ds(pl.multiple_of(step * step_rows, step_rows), step_rows)

    def a_block(step, rel):
        first = pl.multiple_of(across(chip, rel) * span, span)
        return a_ref.at[chunk(step), pl.ds(first, span)]

    def send_first(step):
        send(a_block(step, 7), a_in.at[6, chunk(step)], a_out_sem.at[6], a_in_sem.at[step], across(chip, 7))
        for k, (rel, first, _) in enumerate(TWO_HOP):
            send(a_block(step, rel), a_via.at[k, chunk(step)], a_out_sem.at[k], via_sem.at[step, k], flip(chip, first))
        for k, rel in enumerate((1, 2, 4)):
            send(a_block(step, rel), a_in.at[rel - 1, chunk(step)], a_out_sem.at[3 + k], a_in_sem.at[step], flip(chip, rel))

    def forward(step):
        for k, (rel, _, second) in enumerate(TWO_HOP):
            block = a_via.at[k, chunk(step)]
            wait_bytes(block, via_sem.at[step, k])
            send(block, a_in.at[rel - 1, chunk(step)], a_out_sem.at[7 + k], a_in_sem.at[step], flip(chip, second))

    barrier = pltpu.get_barrier_semaphore()
    for rel in (1, 2, 4, 7):
        pl.semaphore_signal(barrier, inc=1, device_id=device(across(chip, rel), core), device_id_type=MESH)
    pl.semaphore_signal(barrier, inc=1, device_id=device(chip, 1 - core), device_id_type=MESH)
    pl.semaphore_wait(barrier, 5)

    send_first(0)
    send(b_ref, b_in, b_sem.at[0], b_sem.at[1], chip, 1 - core)
    send_first(1)
    for step in range(2):
        forward(step)
        send_first(step + 2)

    def b_copies(block, slot):
        cols = pl.ds(pl.multiple_of(block * COLS, COLS), COLS)
        own = pl.ds(pl.multiple_of(core * depth, depth), depth)
        other = pl.ds(pl.multiple_of((1 - core) * depth, depth), depth)
        return (
            pltpu.make_async_copy(b_ref.at[:, cols], b_vm.at[slot, own], b_load.at[slot]),
            pltpu.make_async_copy(b_in.at[:, cols], b_vm.at[slot, other], b_load.at[slot]),
        )

    wait_bytes(b_in, b_sem.at[1])
    for copy in b_copies(0, 0):
        copy.start()

    def rel_rows(rel):
        return pl.ds(pl.multiple_of(rel * step_rows, step_rows), step_rows)

    def send_parts(unit):
        first, second, third = axes_of(unit)
        slot = unit % 2
        pltpu.make_async_copy(prod.at[slot], part.at[unit], prod_sem.at[slot]).wait()
        for k in range(4):
            rel = first + second * (k // 2) + third * (k % 2)
            send(part.at[unit, rel_rows(rel)], part_in.at[unit, k], part_out_sem, part_in_sem.at[unit], flip(chip, first))

    def multiply(step, _):
        @pl.when((step >= 1) & (step + 1 < STEPS))
        def _():
            forward(step + 1)

        wait_bytes(a_in.at[:, chunk(step)], a_in_sem.at[step])
        pltpu.make_async_copy(a_block(step, 0), a_vm.at[rel_rows(0)], a_load).start()
        for rel in range(1, CHIPS):
            pltpu.make_async_copy(a_in.at[rel - 1, chunk(step)], a_vm.at[rel_rows(rel)], a_load).start()
        wait_bytes(a_vm, a_load)

        def one_unit(block, _):
            unit = step * blocks + block
            slot = unit % 2

            @pl.when(unit + 1 < units)
            def _():
                for copy in b_copies((block + 1) % blocks, 1 - slot):
                    copy.start()

            wait_bytes(b_vm.at[slot], b_load.at[slot])
            prod[slot] = jnp.dot(a_vm[...], b_vm[slot], preferred_element_type=jnp.float32)
            pltpu.make_async_copy(prod.at[slot], part.at[unit], prod_sem.at[slot]).start()

            @pl.when(unit >= 1)
            def _():
                send_parts(unit - 1)

            return 0

        return lax.fori_loop(0, blocks, one_unit, 0)

    lax.fori_loop(0, STEPS, multiply, 0)
    send_parts(units - 1)

    def fetch(unit):
        _, second, third = axes_of(unit)
        slot = unit % 2
        wait_bytes(part_in.at[unit], part_in_sem.at[unit])
        pltpu.make_async_copy(part_in.at[unit], fetched.at[slot, 0], fetch_sem.at[slot]).start()
        for k in range(4):
            rel = second * (k // 2) + third * (k % 2)
            pltpu.make_async_copy(
                part.at[unit, rel_rows(rel)], fetched.at[slot, 1, k], fetch_sem.at[slot]
            ).start()

    fetch(0)

    def add_first(unit, _):
        _, second, _ = axes_of(unit)
        slot = unit % 2

        wait_bytes(fetched.at[slot], fetch_sem.at[slot])
        for k in (2, 3):
            total[unit, k] = fetched[slot, 0, k] + fetched[slot, 1, k]
            send(total.at[unit, k], sum_in.at[unit, k - 2], sum_out_sem, sum_in_sem.at[unit], flip(chip, second))
        @pl.when(unit + 1 < units)
        def _():
            fetch(unit + 1)

        for k in (0, 1):
            total[unit, k] = fetched[slot, 0, k] + fetched[slot, 1, k]
        return 0

    lax.fori_loop(0, units, add_first, 0)

    def add_second(unit, _):
        _, _, third = axes_of(unit)
        wait_bytes(sum_in.at[unit], sum_in_sem.at[unit])
        total[unit, 1] = total[unit, 1] + sum_in[unit, 1]
        send(total.at[unit, 1], last_in.at[unit], last_out_sem, last_in_sem.at[unit], flip(chip, third))
        total[unit, 0] = total[unit, 0] + sum_in[unit, 0]
        return 0

    lax.fori_loop(0, units, add_second, 0)

    def add_last(unit, _):
        wait_bytes(last_in.at[unit], last_in_sem.at[unit])
        c_vm[unit] = (total[unit, 0] + last_in[unit]).astype(c_vm.dtype)
        cols = pl.ds(pl.multiple_of((unit % blocks) * COLS, COLS), COLS)
        pltpu.make_async_copy(c_vm.at[unit], c_ref.at[chunk(unit // blocks), cols], c_sem).start()
        return 0

    lax.fori_loop(0, units, add_last, 0)

    wait_bytes(c_vm, c_sem)
    for k in range(10):
        wait_bytes(a_in.at[0], a_out_sem.at[k])
    wait_bytes(b_ref, b_sem.at[0])
    wait_bytes(part_in, part_out_sem)
    wait_bytes(sum_in, sum_out_sem)
    wait_bytes(last_in, last_out_sem)


def local_product(a_rows, b_rows):
    rows, inner = a_rows.shape
    depth, width = b_rows.shape
    span = inner // CHIPS
    step_rows = rows // STEPS
    units = STEPS * (width // COLS)
    f32, bf16 = jnp.float32, a_rows.dtype
    tile = (step_rows, COLS)
    dma = pltpu.SemaphoreType.DMA
    outs = pl.pallas_call(
        kernel,
        out_shape=[
            jax.ShapeDtypeStruct((rows, width), bf16),
            jax.ShapeDtypeStruct((CHIPS - 1, rows, span), bf16),
            jax.ShapeDtypeStruct((len(TWO_HOP), rows, span), bf16),
            jax.ShapeDtypeStruct((depth, width), bf16),
            jax.ShapeDtypeStruct((units, CHIPS * step_rows, COLS), f32),
            jax.ShapeDtypeStruct((units, 4) + tile, f32),
        ],
        in_specs=[pl.BlockSpec(memory_space=pl.ANY)] * 2,
        out_specs=[pl.BlockSpec(memory_space=pl.ANY)] * 6,
        scratch_shapes=[
            pltpu.VMEM((CHIPS * step_rows, span), bf16),
            pltpu.VMEM((2, span, COLS), bf16),
            pltpu.VMEM((2, CHIPS * step_rows, COLS), f32),
            pltpu.VMEM((units, 4) + tile, f32),
            pltpu.VMEM((2, 2, 4) + tile, f32),
            pltpu.VMEM((units, 2) + tile, f32),
            pltpu.VMEM((units,) + tile, f32),
            pltpu.VMEM((units,) + tile, bf16),
            dma((10,)), dma((STEPS,)), dma((STEPS, len(TWO_HOP))), dma((2,)), dma, dma((2,)), dma((2,)),
            dma, dma((units,)), dma, dma((units,)), dma, dma((units,)),
            dma((2,)), dma,
        ],
        compiler_params=pltpu.CompilerParams(
            collective_id=0, has_side_effects=True, vmem_limit_bytes=67043328
        ),
    )(a_rows, b_rows)
    return outs[0]


def solution(mesh):
    return jax.shard_map(
        local_product,
        mesh=mesh,
        in_specs=(P(("mp", "dp"), None), P(("mp", "dp"), None)),
        out_specs=P(("mp", "dp"), None),
        check_vma=False,
    )
```
